32 devices in a mesh: task: 8 (over z, y), aux: 4 (over x, core).
Axes of the slice: x: 2, y: 2, z: 4, core: 2. Of those that a mesh axis runs over, the one named last changes fastest.
Arguments:
- factors: bfloat16 [8, 2048, 1024], P('task', 'aux'), may hold values from -0.125 to 0.125
- amplitudes: bfloat16 [8, 256, 1024], P('task'), may hold values from -6 to 6
- task_counts: int32 [8], P('task'), may hold values from 1 to 4, 16 in all
- task_tiles: int32 [8, 4, 3], P('task'), may hold values from 0 to 4
Outputs:
- residual: float32 [8, 256, 1024], P('task', None, 'aux')
The draws below stay inside these ranges and needn't reach their ends.
Inputs may be any that keep to these rules, and one draw needn't show every extreme that they name: `task_counts`: every tile has 1 to 4 tasks, exactly 16 in all; some tile has exactly 4.
All inputs are finite; a program needn't handle non-finite values. No bound on the sum of `task_counts` on one device may be relied on, other than what follows from the above.
Results may differ from the reference program's by a relative error of at most 0.0026.
Values may be sent and summed in bfloat16 or wider, within the bound.
A program may use at most 64 MiB of HBM per device.

```python
import math
import jax
import jax.numpy as jnp
import numpy as np
from jax import lax

AUX = 2048
VB = 32
PAIRS = 1024
OCCP = 256
MOST = 4
RADIUS = 2
TILES = 8
TASKS = 16
N_AUX = 4


def place_ends(result, stream_key, smallest, top_value):
    index_at = [jax.random.randint(jax.random.fold_in(stream_key, axis), (), 0, length) for axis, length in enumerate(result.shape)]
    widest = result.shape.index(max(result.shape))
    neighbour = index_at[:widest] + [(index_at[widest] + 1) % result.shape[widest]] + index_at[widest + 1:]
    return result.at[tuple(index_at)].set(smallest).at[tuple(neighbour)].set(top_value)


def steps_of(key, dims, cuts, smallest, top_value):
    gain, own = 1.0, jax.random.fold_in(key, 6)
    for position, shards_of in cuts:
        steps = jnp.exp(jax.random.uniform(jax.random.fold_in(own, position), (shards_of,), jnp.float32, smallest / len(cuts), top_value / len(cuts)))
        gain = gain * jnp.repeat(steps, dims[position] // shards_of).reshape([-1 if axis == position else 1 for axis in range(len(dims))])
    return gain


def profile(count, total, bound, slope):
    weights = [(1 << 20) // math.isqrt(grade ** slope) + 1 for grade in range(2, count + 1)]
    rest, counts = total - bound - (count - 1), [1] * (count - 1)
    while rest > 0:
        movable = [i for i in range(count - 1) if counts[i] < bound]
        pool, remaining = sum([weights[i] for i in movable]), rest
        for i in movable:
            addition = min(bound - counts[i], max(1, remaining * weights[i] // pool), rest)
            counts[i] = counts[i] + addition
            rest = rest - addition
    return np.array([bound] + counts)


def uneven(stream_key, amount, total, bound, skew):
    if amount == 2:
        one = jax.random.randint(stream_key, (), max(1, total - bound), min(bound, total - 1) + 1)
        return jnp.stack([one, total - one])
    tallies = jnp.asarray(profile(amount, total, bound, skew), jnp.int32)
    pairs = (amount - 1) // 2
    giver, sink = tallies[1:1 + 2 * pairs:2], tallies[2:2 + 2 * pairs:2]
    margin = jnp.minimum(giver - 1, bound - sink)
    moved = jax.random.randint(jax.random.fold_in(stream_key, 1), (pairs,), 0, 1 << 20) % (margin + 1)
    tallies = tallies.at[1:1 + 2 * pairs:2].set(giver - moved).at[2:2 + 2 * pairs:2].set(sink + moved)
    return tallies[jax.random.permutation(jax.random.fold_in(stream_key, 2), amount)]


def gaussian(own_key, dims, spread, reach, shards=(), kind=jnp.bfloat16):
    result = jax.random.normal(own_key, dims, jnp.float32) * spread
    if len(shards) > 0:
        result = steps_of(own_key, dims, shards, -0.22, 0.18) * result
    return jnp.clip(result, min=-reach, max=reach).astype(kind)


def setup_inputs(seed: int = 0) -> dict:
    seeds = jax.random.split(jax.random.key(seed), 5)
    return {
        "factors": gaussian(seeds[0], (TILES, AUX, PAIRS), AUX ** -0.5, 0.125, ((0, 8), (1, 4))),
        "amplitudes": gaussian(seeds[1], (TILES, OCCP, PAIRS), 1.0, 6.0, ((0, 8),)),
        "task_counts": uneven(seeds[2], TILES, TASKS, MOST, 2).astype(jnp.int32),
        "task_tiles": place_ends(jax.random.randint(seeds[3], (TILES, MOST, 3), 0, 2 * RADIUS + 1), jax.random.fold_in(seeds[3], 1), 0, 2 * RADIUS).astype(jnp.int32),
    }


def quarter_term(first, second, amp):
    tile = lax.dot_general(first, second, (((0,), (0,)), ((), ())), preferred_element_type=jnp.float32)
    tile = tile.reshape(VB, VB, VB, VB).transpose(1, 3, 0, 2).reshape(VB * VB, VB * VB)
    tile = tile.astype(jnp.bfloat16)
    return jnp.dot(amp, tile, preferred_element_type=jnp.float32)


def task_term(first, second, amp):
    width = AUX // N_AUX
    total = jnp.zeros((amp.shape[0], VB * VB), jnp.float32)
    for quarter in range(N_AUX):
        lower = quarter * width
        total = total + quarter_term(first[lower:lower + width], second[lower:lower + width], amp)
    return total


def reference(factors, amplitudes, task_counts, task_tiles):
    owners = jnp.repeat(jnp.arange(TILES, dtype=jnp.int32), MOST)
    slots = jnp.tile(jnp.arange(MOST, dtype=jnp.int32), TILES)

    def step(total, item):
        owner, slot = item
        offs = task_tiles[owner, slot]
        idx = (owner + offs - RADIUS) % TILES
        live = slot < task_counts[owner]

        def compute(unused):
            return task_term(factors[idx[0]], factors[idx[1]], amplitudes[idx[2]])

        def empty(unused):
            return jnp.zeros((OCCP, VB * VB), jnp.float32)

        term = lax.cond(live, compute, empty, 0)
        total = lax.dynamic_update_index_in_dim(total, lax.dynamic_index_in_dim(total, owner, 0, False) + term, owner, 0)
        return total, 0

    start = jnp.zeros((TILES, OCCP, VB * VB), jnp.float32)
    total, unused = lax.scan(step, start, (owners, slots))
    return total
```

```python
import jax
import jax.numpy as jnp
from jax import lax
from jax.experimental import pallas as pl
from jax.experimental.pallas import tpu as pltpu
from jax.sharding import PartitionSpec as P

VB = 32
RADIUS = 2
SPAN = 2 * RADIUS + 1
LANES = 128
SPREAD = LANES // VB
STEP = 2


def shifted(block, axis, distance):
    devices = range(lax.axis_size(axis))
    route = [((i - distance) % len(devices), i) for i in devices]
    return lax.ppermute(block, axis, route)


def swap_matrix(width):
    pairs = width * width
    rows = lax.broadcasted_iota(jnp.int32, (pairs, pairs), 0)
    cols = lax.broadcasted_iota(jnp.int32, (pairs, pairs), 1)
    return (rows == (cols % width) * width + cols // width).astype(jnp.bfloat16)


def roll_groups(x, amount):
    if amount == 0:
        return x
    parts = [
        pltpu.roll(x[:, j * LANES : (j + 1) * LANES], amount, 1)
        for j in range(x.shape[1] // LANES)
    ]
    return jnp.concatenate(parts, axis=1)


def kernel(counts, plan, swap, *refs):
    fac_in, amp_in = refs[:SPAN], refs[SPAN : 2 * SPAN]
    out, fac, amp, flip, tile, sems = refs[2 * SPAN :]
    pairs = swap.shape[0]
    blocks = pairs // LANES
    copies = [pltpu.make_async_copy(fac_in[i], fac.at[i], sems.at[i]) for i in range(SPAN)]
    copies += [
        pltpu.make_async_copy(amp_in[i], amp.at[i], sems.at[SPAN + i]) for i in range(SPAN)
    ]
    for copy in copies:
        copy.start()
    out[...] = jnp.zeros_like(out)
    for copy in copies:
        copy.wait()
    lanes = STEP * LANES
    group = (lax.broadcasted_iota(jnp.int32, (VB * blocks, lanes), 1) // VB) % SPREAD

    @pl.loop(0, counts[0])
    def _(slot):
        left, right, third = plan[slot, 0], plan[slot, 1], plan[slot, 2]
        for a_hi in range(blocks):
            strip = fac[left, :, a_hi * LANES : (a_hi + 1) * LANES].T
            for s in range(SPREAD):
                flip[s, a_hi * VB : (a_hi + 1) * VB, :] = strip[s * VB : (s + 1) * VB, :]

        @pl.loop(0, blocks // STEP)
        def _(step):
            base = pl.multiple_of(step * lanes, lanes)
            cols = swap[:, pl.ds(base, lanes)]
            swapped = jnp.dot(fac[right], cols, preferred_element_type=jnp.float32)
            outs = []
            for s in range(SPREAD):
                turned = roll_groups(swapped, s * VB).astype(jnp.bfloat16)
                outs.append(jnp.dot(flip[s], turned, preferred_element_type=jnp.float32))
            for t in range(SPREAD):
                mixed = outs[(SPREAD - 1 - t) % SPREAD]
                for g in range(SPREAD - 1):
                    mixed = jnp.where(group == g, outs[(g - t) % SPREAD], mixed)
                mixed = roll_groups(mixed, (LANES - t * VB) % LANES).astype(jnp.bfloat16)
                for j in range(STEP):
                    row = pl.multiple_of(base + (j * SPREAD + t) * VB, VB)
                    for a_hi in range(blocks):
                        tile[pl.ds(row, VB), a_hi * LANES : (a_hi + 1) * LANES] = mixed[
                            a_hi * VB : (a_hi + 1) * VB, j * LANES : (j + 1) * LANES
                        ]

        @pl.loop(0, blocks // STEP)
        def _(step):
            base = pl.multiple_of(step * lanes, lanes)
            amps = jnp.dot(
                amp[third], swap[:, pl.ds(base, lanes)], preferred_element_type=jnp.float32
            ).astype(jnp.bfloat16)
            out[...] += jnp.dot(
                amps, tile[pl.ds(base, lanes), :], preferred_element_type=jnp.float32
            )


def run_tasks(facs, amps, counts, plan):
    depth, pairs = facs[0].shape
    occ = amps[0].shape[0]
    anywhere = pl.BlockSpec(memory_space=pl.ANY)
    scalars = pl.BlockSpec(memory_space=pltpu.SMEM)
    return pl.pallas_call(
        kernel,
        out_shape=jax.ShapeDtypeStruct((occ, pairs), jnp.float32),
        in_specs=[scalars, scalars, pl.BlockSpec(memory_space=pltpu.VMEM)]
        + [anywhere] * (2 * SPAN),
        out_specs=pl.BlockSpec(memory_space=pltpu.VMEM),
        scratch_shapes=[
            pltpu.VMEM((SPAN, depth, pairs), jnp.bfloat16),
            pltpu.VMEM((SPAN, occ, pairs), jnp.bfloat16),
            pltpu.VMEM((SPREAD, pairs // SPREAD, depth), jnp.bfloat16),
            pltpu.VMEM((pairs, pairs), jnp.bfloat16),
            pltpu.SemaphoreType.DMA((2 * SPAN,)),
        ],
        compiler_params=pltpu.CompilerParams(vmem_limit_bytes=48 * 1024 * 1024),
    )(counts, plan, swap_matrix(VB), *facs, *amps)


def shards(factors, amplitudes, task_counts, task_tiles):
    own_fac = factors[0]
    own_amp = amplitudes[0]
    facs = []
    amps = []
    for offset in range(-RADIUS, RADIUS + 1):
        if offset == 0:
            facs.append(own_fac)
            amps.append(own_amp)
        else:
            moved = shifted((own_fac, own_amp), "task", -offset)
            facs.append(moved[0])
            amps.append(moved[1])
    partial_sum = run_tasks(facs, amps, task_counts, task_tiles[0])
    summed = lax.psum_scatter(partial_sum, "aux", scatter_dimension=1, tiled=True)
    return summed[None]


def solution(mesh):
    return jax.shard_map(
        shards,
        mesh=mesh,
        in_specs=(P("task", "aux", None), P("task", None, None), P("task"), P("task", None, None)),
        out_specs=P("task", None, "aux"),
        check_vma=False,
    )
```
